32 devices in a mesh: mode: 8 (over z, y), cores: 4 (over x, core).
Axes of the slice: x: 2, y: 2, z: 4, core: 2. Of those that a mesh axis runs over, the one named last changes fastest.
Arguments:
- train_cores: bfloat16 [4, 400, 32, 400], P('cores', None, 'mode'), may hold values from -0.24748737 to 0.24748737
- sketch_cores: bfloat16 [4, 100, 32, 100], P('cores', None, 'mode'), may hold values from -0.3125 to 0.3125
- left_interface: float32 [100, 400], replicated, may hold values from -6 to 6
- right_sketch: bfloat16 [400, 100], replicated, may hold values from -6 to 6
Outputs:
- frames: bfloat16 [4, 100, 32, 100], P('cores', None, 'mode')
- interfaces: float32 [4, 100, 400], P('cores')
The draws below stay inside these ranges and needn't reach their ends.
All inputs are finite; a program needn't handle non-finite values.
Results may differ from the reference program's by a relative error of at most 0.019.
Values may be sent and summed in bfloat16 or wider, within the bound.
A program may use at most 64 MiB of HBM per device.

```python
import math
import jax
import jax.numpy as jnp
from jax import lax

RANK = 400
SKETCH = 100
MODE = 32
CHAIN = 4


def draw_train_cores(key, part):
    key_scale = jax.random.fold_in(key, 11)
    key_entry = jax.random.fold_in(key, 12)
    exponent = jax.random.uniform(key_scale, (CHAIN, 1, MODE, 1), jnp.float32)
    factor = jnp.exp(exponent * math.log(10.0)) / 4.6
    entries = jnp.clip(jax.random.normal(key_entry, (CHAIN, RANK, MODE, RANK), jnp.float32), -6.0, 6.0)
    return (entries * factor / math.sqrt(MODE * SKETCH)).astype(jnp.bfloat16)


def levels(key, dims, cuts, smallest, largest):
    gain, own = 1.0, jax.random.fold_in(key, 6)
    for position, parts in cuts:
        heights = jnp.exp(jax.random.uniform(jax.random.fold_in(own, position), (parts,), jnp.float32, smallest / len(cuts), largest / len(cuts)))
        gain = gain * jnp.repeat(heights, dims[position] // parts).reshape([-1 if axis == position else 1 for axis in range(len(dims))])
    return gain


def gaussian(stream_key, shape, deviation, limit, shards=(), kind=jnp.bfloat16):
    values = deviation * jax.random.normal(stream_key, shape, jnp.float32)
    if shards:
        values = values * levels(stream_key, shape, shards, -0.22, 0.18)
    return jnp.clip(values, -limit, limit).astype(kind)


def setup_inputs(seed: int = 0) -> dict:
    keys = jax.random.split(jax.random.key(seed), 5)
    return {
        "train_cores": draw_train_cores(jax.random.fold_in(keys[4], 71), 0),
        "sketch_cores": gaussian(keys[1], (CHAIN, SKETCH, MODE, SKETCH), RANK ** -0.5, 0.3125, ((0, 4), (2, 8))),
        "left_interface": gaussian(keys[2], (SKETCH, RANK), 1.0, 6.0, (), jnp.float32),
        "right_sketch": gaussian(keys[3], (RANK, SKETCH), 1.0, 6.0),
    }


def reference(train_cores, sketch_cores, left_interface, right_sketch):
    sketches = [right_sketch]
    for index in range(CHAIN - 1, 0, -1):
        flat_core = train_cores[index].reshape(RANK * MODE, RANK)
        partial_value = jnp.dot(flat_core.astype(jnp.float32), sketches[0].astype(jnp.float32), preferred_element_type=jnp.float32).astype(jnp.bfloat16)
        partial_value = partial_value.reshape(RANK, MODE * SKETCH)
        sketch_flat = sketch_cores[index].reshape(SKETCH, MODE * SKETCH)
        next_sketch = lax.dot_general(partial_value.astype(jnp.float32), sketch_flat.astype(jnp.float32), (((1,), (1,)), ((), ())), preferred_element_type=jnp.float32)
        sketches.insert(0, next_sketch.astype(jnp.bfloat16))
    frame_scale = math.sqrt(SKETCH * MODE)
    carry = left_interface
    frame_list = []
    carry_list = []
    for index in range(CHAIN):
        carry_low = carry.astype(jnp.bfloat16)
        built = jnp.dot(carry_low.astype(jnp.float32), train_cores[index].reshape(RANK, MODE * RANK).astype(jnp.float32), preferred_element_type=jnp.float32)
        built = built.astype(jnp.bfloat16).reshape(SKETCH * MODE, RANK)
        images = jnp.dot(built.astype(jnp.float32), sketches[index].astype(jnp.float32), preferred_element_type=jnp.float32)
        gram_matrix = lax.dot_general(images, images, (((0,), (0,)), ((), ())), precision=lax.Precision.HIGHEST)
        chol_lower = jnp.linalg.cholesky(gram_matrix)
        frame_rows = lax.linalg.triangular_solve(chol_lower, images.T, left_side=True, lower=True)
        frame_list.append((frame_rows.T * frame_scale).astype(jnp.bfloat16).reshape(SKETCH, MODE, SKETCH))
        carry = jnp.dot(frame_rows, built.astype(jnp.float32), precision=lax.Precision.HIGHEST)
        carry_list.append(carry)
    return (jnp.stack(frame_list), jnp.stack(carry_list))
```

```python
import functools
import math

import jax
import jax.numpy as jnp
from jax import lax
from jax.experimental import pallas as pl
from jax.experimental.pallas import tpu as pltpu
from jax.sharding import PartitionSpec as P

MESH = pl.DeviceIdType.MESH
F32, BF16 = jnp.float32, jnp.bfloat16
EXACT = lax.Precision.HIGHEST
LANES = 128


def up(value, step):
    return -(-value // step) * step


def dot(a, b, ca, cb, precision=None):
    return lax.dot_general(
        a, b, (((ca,), (cb,)), ((), ())), preferred_element_type=F32, precision=precision
    )


def partner(me, d, size):
    if size & (size - 1):
        return lax.rem(me + d, size)
    other, bit = 0, 1
    while bit < size:
        digit = lax.rem(lax.div(me, bit), 2)
        other = other + bit * ((1 - digit) if d & bit else digit)
        bit *= 2
    return other


def far_first(size):
    return list(range(size - 1, 0, -1))


def owner_first(size):
    order = far_first(size)
    half = size // 2
    middle = [d for d in order if d >= half and d < half + half // 2]
    return middle + [d for d in order if d not in middle]


def lower_inverse(gram, size, look=4):
    full = gram.shape[0]
    lane = lax.broadcasted_iota(jnp.int32, (1, full), 1)
    top, table, done = 0, gram, []
    for first in range(0, size, look):
        base = first // 8 * 8
        if base > top:
            done.append(table[: base - top])
            table = table[base - top :]
            top = base
        rows = full - top
        width = min(look, size - first)
        row_id = lax.broadcasted_iota(jnp.int32, (rows, full), 0) + top
        columns = [
            jnp.broadcast_to(table[:, first + t : first + t + 1], (rows, full)) for t in range(width)
        ]
        for t in range(width):
            j = first + t
            here = j - top
            column = columns[t]
            pivot = column[here : here + 1]
            inverse = 1.0 / pivot
            row = jnp.where(lane == j, 1.0, table[here : here + 1]) * inverse
            below = row_id > j
            lower = jnp.where(below, column, 0.0)
            for s in range(t + 1, width):
                ahead = here + s - t
                columns[s] = columns[s] - lower * (column[ahead : ahead + 1] * inverse)
            table = jnp.where((lane == j) & below, 0.0, table) - lower * row
    done.append(table)
    table = jnp.concatenate(done, axis=0) if len(done) > 1 else table
    row_id = lax.broadcasted_iota(jnp.int32, (full, full), 0)
    lane = lax.broadcasted_iota(jnp.int32, (full, full), 1)
    pivots = jnp.sum(jnp.where(row_id == lane, table, 0.0), axis=1, keepdims=True)
    unit = jnp.where(row_id > lane, table, jnp.where(row_id == lane, 1.0, 0.0))
    return unit * lax.rsqrt(pivots)


def kernel(
    dims,
    core_hbm,
    gauss_hbm,
    left_hbm,
    right_hbm,
    frames_ref,
    faces_ref,
    core_ref,
    gauss_ref,
    left_ref,
    right_ref,
    slices,
    gauss,
    rows_buf,
    sketch_buf,
    part_out,
    part_in,
    carry_buf,
    carry_own,
    proj_out,
    proj_in,
    gram_out,
    gram_in,
    piece_sk,
    piece_ca,
    s_load,
    s_part,
    r_part,
    s_sk,
    r_sk,
    s_proj,
    r_proj,
    s_gram,
    r_gram,
    s_next,
    r_next,
    s_own,
    r_own,
):
    size, group_count, rank, sketch, modes, owners, scale = dims
    wide = sketch_buf.shape[1]
    tall = carry_buf.shape[1]
    me = lax.axis_index("mode")
    group = lax.axis_index("cores")
    final = group_count - 1
    first = (size - owners) // 2
    down = lax.rem(group + group_count - 1, group_count)
    upward = lax.rem(group + 1, group_count)
    extents = [min(LANES, up(rank - LANES * c, 16)) for c in range(owners)]
    last = first + owners - 1
    owner = (me >= first) & (me <= last)
    mine = jnp.clip(me - first, 0, owners - 1)

    barrier = pltpu.get_barrier_semaphore()

    def greet(peer, to_group):
        pl.semaphore_signal(
            barrier, inc=1, device_id={"mode": peer, "cores": to_group}, device_id_type=MESH
        )

    for d in far_first(size):
        greet(partner(me, d, size), group)
    for c in range(owners):
        pl.when(group < final)(lambda c=c: greet(first + c, upward))
        pl.when(group > 0)(lambda c=c: greet(first + c, down))

    loads = [
        pltpu.make_async_copy(src, dst, s_load.at[n])
        for n, (src, dst) in enumerate(
            [(right_hbm, right_ref), (core_hbm, core_ref), (gauss_hbm, gauss_ref), (left_hbm, left_ref)]
        )
    ]
    for load in loads:
        load.start()

    def meet():
        sides = (group > 0).astype(jnp.int32) + (group < final).astype(jnp.int32)
        pl.semaphore_wait(barrier, size - 1 + size * sides * owner.astype(jnp.int32))

    def scatter(out_ref, in_ref, sends, recvs):
        return [
            pltpu.make_async_remote_copy(
                src_ref=out_ref.at[pl.ds(c * LANES, extents[c])],
                dst_ref=in_ref.at[me, pl.ds(0, extents[c])],
                send_sem=sends.at[c],
                recv_sem=recvs.at[me],
                device_id={"mode": first + c},
                device_id_type=MESH,
            )
            for c in range(owners)
        ]

    def scatter_start(copies):
        def go(order):
            for c in order:
                pl.when(me != first + c)(lambda c=c: copies[c].start())

        pl.when(me < size // 2)(lambda: go(range(owners - 1, -1, -1)))
        pl.when(me >= size // 2)(lambda: go(range(owners)))

    def scatter_sent(copies):
        for c in range(owners):
            pl.when(me != first + c)(lambda c=c: copies[c].wait_send())

    def gathered(out_ref, in_ref, recvs, extent):
        value = out_ref[pl.ds(pl.multiple_of(mine * LANES, LANES), extent)].astype(F32)
        for d in far_first(size)[::-1]:
            peer = partner(me, d, size)
            landing = in_ref.at[peer, pl.ds(0, extent)]
            pltpu.make_async_remote_copy(
                src_ref=landing,
                dst_ref=landing,
                send_sem=recvs.at[peer],
                recv_sem=recvs.at[peer],
                device_id={"mode": partner(me, 1, size)},
                device_id_type=MESH,
            ).wait_recv()
            value = value + landing[...].astype(F32)
        return value

    def spread(src_ref, dst_ref, sends, recvs, to_group, home):
        return [
            pltpu.make_async_remote_copy(
                src_ref=src_ref,
                dst_ref=dst_ref,
                send_sem=sends.at[d],
                recv_sem=recvs.at[mine],
                device_id={"mode": partner(me, d, size), "cores": to_group},
                device_id_type=MESH,
            )
            for d in owner_first(size) + ([0] if home else [])
        ]

    def await_piece(dst_ref, recvs, c):
        pltpu.make_async_remote_copy(
            src_ref=dst_ref,
            dst_ref=dst_ref,
            send_sem=recvs.at[c],
            recv_sem=recvs.at[c],
            device_id={"mode": partner(me, 1, size)},
            device_id_type=MESH,
        ).wait_recv()

    def owned(run):
        if extents[-1] == LANES:
            pl.when(owner)(lambda: run(LANES))
        else:
            pl.when(owner & (me < last))(lambda: run(LANES))
            pl.when(me == last)(lambda: run(extents[-1]))

    def split():
        for i in range(modes):
            slices[i] = core_ref[:, i, :]

    part_out[...] = jnp.zeros(part_out.shape, part_out.dtype)
    if proj_out.shape[0] > rank:
        proj_out[pl.ds(rank, proj_out.shape[0] - rank), :] = jnp.zeros(
            (proj_out.shape[0] - rank, wide), F32
        )
    loads[2].wait()
    for i in range(modes):
        gauss[i] = gauss_ref[:, i, :]
    loads[0].wait()
    loads[1].wait()
    loads[3].wait()

    @pl.when(group == final)
    def _():
        sketch_buf[...] = jnp.zeros(sketch_buf.shape, BF16)
        sketch_buf[pl.ds(0, rank), pl.ds(0, sketch)] = right_ref[...]

    @pl.when(group < final)
    def _():
        split()
        meet()
        for c in range(owners):
            await_piece(sketch_buf.at[pl.ds(c * LANES, extents[c])], r_sk, c)

    part_copies = scatter(part_out, part_in, s_part, r_part)
    held = sketch_buf[pl.ds(0, rank), :]
    rows_buf[...] = dot(core_ref[...].reshape(rank * modes, rank), held, 1, 0)
    partials = [rows_buf[pl.ds(i, rank, stride=modes), :].astype(BF16) for i in range(modes)]

    @pl.when(group > 0)
    def _():
        total = None
        for i in range(modes):
            term = dot(partials[i][:, :sketch], gauss[i], 1, 1)
            total = term if total is None else total + term
        part_out[pl.ds(0, rank), pl.ds(0, sketch)] = total.astype(part_out.dtype)
        pl.when(group == final)(meet)
        scatter_start(part_copies)

        def finish(extent):
            piece = piece_sk.at[pl.ds(0, extent)]
            target = sketch_buf.at[pl.ds(pl.multiple_of(mine * LANES, LANES), extent)]
            copies = spread(piece, target, s_sk, r_sk, down, True)
            piece[...] = gathered(part_out, part_in, r_part, extent).astype(BF16)
            for copy in copies:
                copy.start()
            for copy in copies:
                copy.wait_send()

        owned(finish)
        scatter_sent(part_copies)

    pl.when(group == final)(split)

    @pl.when(group == 0)
    def _():
        carry_buf[...] = jnp.zeros(carry_buf.shape, BF16)
        carry = left_ref[...].T.astype(BF16)
        for c in range(owners):
            width = min(LANES, rank - c * LANES)
            carry_buf[c, pl.ds(0, sketch), pl.ds(0, width)] = carry[:, c * LANES : c * LANES + width]

    @pl.when(group > 0)
    def _():
        for c in range(owners):
            await_piece(carry_buf.at[c], r_next, c)

    carry = jnp.concatenate([carry_buf[c] for c in range(owners)], axis=1)[:, :rank]
    gram_copies = [
        pltpu.make_async_remote_copy(
            src_ref=gram_out,
            dst_ref=gram_in.at[me],
            send_sem=s_gram.at[d],
            recv_sem=r_gram.at[me],
            device_id={"mode": partner(me, d, size)},
            device_id_type=MESH,
        )
        for d in far_first(size)
    ]
    proj_copies = scatter(proj_out, proj_in, s_proj, r_proj)
    images = [dot(carry, partials[i], 1, 0) for i in range(modes)]
    image = jnp.concatenate(images, axis=0)
    high = image.astype(BF16)
    low = (image - high.astype(F32)).astype(BF16)
    pair = jnp.concatenate([high, low], axis=1)
    terms = dot(high, pair, 0, 0)
    cross = terms[:, wide:]
    gram = terms[:, :wide] + cross + cross.T
    half, quarter = wide // 2, wide // 4
    lower_rows = gram_out.shape[0] - quarter
    gram_out[pl.ds(0, lower_rows), :] = gram[half : half + lower_rows]
    gram_out[pl.ds(lower_rows, quarter), :] = jnp.concatenate(
        [gram[:quarter, :half], gram[quarter:half, :half]], axis=1
    )
    for copy in gram_copies:
        copy.start()
    built = jnp.concatenate(
        [dot(carry, slices[i], 1, 0).astype(BF16) for i in range(modes)], axis=0
    )
    proj = dot(built, pair, 0, 0)
    proj_out[pl.ds(0, rank), :] = proj[:, :wide] + proj[:, wide:]
    scatter_start(proj_copies)

    gram_in[me] = gram_out[...]
    for d in far_first(size)[::-1]:
        peer = partner(me, d, size)
        await_piece(gram_in.at[peer], r_gram, peer)
    total = None
    for source in range(size):
        term = gram_in[source]
        total = term if total is None else total + term
    lower = total[:lower_rows]
    if lower_rows < half:
        lower = jnp.concatenate([lower, jnp.zeros((half - lower_rows, wide), F32)], axis=0)
    corner = total[lower_rows:]
    corner = jnp.concatenate([corner[:, :half], corner[:, half:]], axis=0)
    upper = jnp.concatenate([corner, lower.T[:half]], axis=1)
    total = jnp.concatenate([upper, lower], axis=0)
    row_id = lax.broadcasted_iota(jnp.int32, (wide, wide), 0)
    lane_id = lax.broadcasted_iota(jnp.int32, (wide, wide), 1)
    total = jnp.where((row_id == lane_id) & (row_id >= sketch), 1.0, total)
    inverse = lower_inverse(total, sketch, 8)

    next_copies = spread(piece_ca, carry_buf.at[mine], s_next, r_next, upward, True)
    own_copies = spread(piece_ca, carry_own.at[mine], s_own, r_own, group, False)

    def project(extent):
        value = gathered(proj_out, proj_in, r_proj, extent)
        if extent < LANES:
            value = jnp.concatenate([value, jnp.zeros((LANES - extent, wide), F32)], axis=0)
        piece_ca[...] = dot(inverse, value, 1, 1, EXACT)[:tall].astype(BF16)

        @pl.when(group < final)
        def _():
            for copy in next_copies:
                copy.start()

        for copy in own_copies:
            copy.start()
        carry_own[mine] = piece_ca[...]

    owned(project)
    orth = dot(image, inverse, 1, 1, EXACT) * scale
    for i in range(modes):
        rows_buf[pl.ds(i, tall, stride=modes), :] = orth[i * tall : (i + 1) * tall]
    frames = rows_buf[pl.ds(0, sketch * modes), :].astype(BF16)
    frames_ref[...] = frames[:, :sketch].reshape(sketch, modes, sketch)
    scatter_sent(proj_copies)
    for copy in gram_copies:
        copy.wait_send()
    for c in range(owners):

        @pl.when(me != first + c)
        def _(c=c):
            await_piece(carry_own.at[c], r_own, c)

    faces = jnp.concatenate([carry_own[c] for c in range(owners)], axis=1)
    faces_ref[...] = faces[:sketch, :rank].astype(F32).reshape(sketch, 1, rank)

    def drain():
        for copy in own_copies:
            copy.wait_send()

        @pl.when(group < final)
        def _():
            for copy in next_copies:
                copy.wait_send()

    pl.when(owner)(drain)


def body(train_cores, sketch_cores, left_interface, right_sketch):
    size = lax.axis_size("mode")
    group_count = lax.axis_size("cores")
    _, rank, modes, _ = train_cores.shape
    sketch = sketch_cores.shape[1]
    wide, tall = up(sketch, LANES), up(sketch, 8)
    owners = -(-rank // LANES)
    deep = owners * LANES
    scale = math.sqrt(sketch * modes * size)
    dims = (size, group_count, rank, sketch, modes, owners, scale)
    gram_rows = up(max(sketch - wide // 2, 8), 8) + wide // 4
    anywhere = pl.BlockSpec(memory_space=pl.ANY)
    vmem = pl.BlockSpec(memory_space=pltpu.VMEM)
    dma = pltpu.SemaphoreType.DMA((size,))
    frames, faces = pl.pallas_call(
        functools.partial(kernel, dims),
        out_shape=(
            jax.ShapeDtypeStruct((sketch, modes, sketch), BF16),
            jax.ShapeDtypeStruct((sketch, 1, rank), F32),
        ),
        in_specs=[anywhere] * 4,
        out_specs=(vmem, vmem),
        scratch_shapes=[
            pltpu.VMEM((rank, modes, rank), BF16),
            pltpu.VMEM((sketch, modes, sketch), BF16),
            pltpu.VMEM((rank, sketch), F32),
            pltpu.VMEM((rank, sketch), BF16),
            pltpu.VMEM((modes, rank, rank), BF16),
            pltpu.VMEM((modes, sketch, sketch), BF16),
            pltpu.VMEM((rank * modes, wide), F32),
            pltpu.VMEM((deep, wide), BF16),
            pltpu.VMEM((deep, wide), BF16),
            pltpu.VMEM((size, LANES, wide), BF16),
            pltpu.VMEM((owners, tall, LANES), BF16),
            pltpu.VMEM((owners, tall, LANES), BF16),
            pltpu.VMEM((deep, wide), F32),
            pltpu.VMEM((size, LANES, wide), F32),
            pltpu.VMEM((gram_rows, wide), F32),
            pltpu.VMEM((size, gram_rows, wide), F32),
            pltpu.VMEM((LANES, wide), BF16),
            pltpu.VMEM((tall, LANES), BF16),
        ]
        + [dma] * 13,
        compiler_params=pltpu.CompilerParams(collective_id=0, has_side_effects=True),
    )(train_cores[0], sketch_cores[0], left_interface.T, right_sketch)
    return frames[None], faces[:, 0][None]


def solution(mesh):
    in_specs = (P("cores", None, "mode", None), P("cores", None, "mode", None), P(), P())
    out_specs = (P("cores", None, "mode", None), P("cores", None, None))
    return jax.shard_map(body, mesh=mesh, in_specs=in_specs, out_specs=out_specs, check_vma=False)
```

```python
import contextlib
import functools
import math

import jax
import jax.numpy as jnp
from jax import lax
from jax.experimental import pallas as pl
from jax.experimental.pallas import tpu as pltpu
from jax.sharding import PartitionSpec as P

MESH = pl.DeviceIdType.MESH
F32, BF16 = jnp.float32, jnp.bfloat16
EXACT = lax.Precision.HIGHEST
LANES = 128
scope = contextlib.nullcontext


def up(value, step):
    return -(-value // step) * step


def dot(a, b, ca, cb, precision=None):
    return lax.dot_general(
        a, b, (((ca,), (cb,)), ((), ())), preferred_element_type=F32, precision=precision
    )


def partner(me, d, size):
    if size & (size - 1):
        return lax.rem(me + d, size)
    other, bit = 0, 1
    while bit < size:
        digit = lax.rem(lax.div(me, bit), 2)
        other = other + bit * ((1 - digit) if d & bit else digit)
        bit *= 2
    return other


def far_first(size):
    return list(range(size - 1, 0, -1))


def owner_first(size):
    order = far_first(size)
    half = size // 2
    middle = [d for d in order if d >= half and d < half + half // 2]
    return middle + [d for d in order if d not in middle]


def lower_inverse(gram, size, look=4):
    full = gram.shape[0]
    lane = lax.broadcasted_iota(jnp.int32, (1, full), 1)
    top, table, done = 0, gram, []
    for first in range(0, size, look):
        base = first // 8 * 8
        if base > top:
            done.append(table[: base - top])
            table = table[base - top :]
            top = base
        rows = full - top
        width = min(look, size - first)
        row_id = lax.broadcasted_iota(jnp.int32, (rows, full), 0) + top
        columns = [
            jnp.broadcast_to(table[:, first + t : first + t + 1], (rows, full)) for t in range(width)
        ]
        for t in range(width):
            j = first + t
            here = j - top
            column = columns[t]
            pivot = column[here : here + 1]
            inverse = 1.0 / pivot
            row = jnp.where(lane == j, 1.0, table[here : here + 1]) * inverse
            below = row_id > j
            lower = jnp.where(below, column, 0.0)
            for s in range(t + 1, width):
                ahead = here + s - t
                columns[s] = columns[s] - lower * (column[ahead : ahead + 1] * inverse)
            table = jnp.where((lane == j) & below, 0.0, table) - lower * row
    done.append(table)
    table = jnp.concatenate(done, axis=0) if len(done) > 1 else table
    row_id = lax.broadcasted_iota(jnp.int32, (full, full), 0)
    lane = lax.broadcasted_iota(jnp.int32, (full, full), 1)
    pivots = jnp.sum(jnp.where(row_id == lane, table, 0.0), axis=1, keepdims=True)
    unit = jnp.where(row_id > lane, table, jnp.where(row_id == lane, 1.0, 0.0))
    return unit * lax.rsqrt(pivots)


def kernel(
    dims,
    core_hbm,
    gauss_hbm,
    left_hbm,
    right_hbm,
    frames_ref,
    faces_ref,
    core_ref,
    gauss_ref,
    left_ref,
    right_ref,
    slices,
    gauss,
    rows_buf,
    sketch_buf,
    head_buf,
    part_out,
    part_in,
    head_in,
    carry_buf,
    carry_own,
    proj_out,
    proj_in,
    gram_out,
    gram_in,
    piece_sk,
    piece_ca,
    piece_hd,
    inv_buf,
    inv_in,
    wide_out,
    wide_in,
    wide_piece,
    wide_all,
    full_hi,
    full_lo,
    s_load,
    s_part,
    r_part,
    r_head,
    s_sk,
    r_sk,
    s_hd,
    r_hd,
    s_proj,
    r_proj,
    s_gram,
    r_gram,
    s_next,
    r_next,
    s_own,
    r_own,
    s_wide,
    r_wide,
    s_all,
    r_all,
    s_twin,
    r_twin,
):
    size, group_count, rank, sketch, modes, owners, scale = dims
    wide = sketch_buf.shape[1]
    tall = carry_buf.shape[1]
    share = wide_piece.shape[0]
    me = lax.axis_index("mode")
    group = lax.axis_index("cores")
    final = group_count - 1
    first = (size - owners) // 2
    down = lax.rem(group + group_count - 1, group_count)
    upward = lax.rem(group + 1, group_count)
    extents = [min(LANES, up(rank - LANES * c, 16)) for c in range(owners)]
    last = first + owners - 1
    owner = (me >= first) & (me <= last)
    mine = jnp.clip(me - first, 0, owners - 1)
    everyone = [0] + far_first(size)[::-1]

    barrier = pltpu.get_barrier_semaphore()

    def greet(peer, to_group):
        pl.semaphore_signal(
            barrier, inc=1, device_id={"mode": peer, "cores": to_group}, device_id_type=MESH
        )

    @pl.when(group > 0)
    def _():
        for d in far_first(size):
            greet(partner(me, d, size), group)

    @pl.when(group > 1)
    def _():
        for c in range(owners):
            greet(first + c, down)

    @pl.when((group > 0) & (group < final) & owner)
    def _():
        for d in range(size):
            greet(partner(me, d, size), upward)

    @pl.when(group == 1)
    def _():
        for d in range(size):
            greet(partner(me, d, size), down)

    pl.when(group == 0)(lambda: greet(me, upward))

    loads = [
        pltpu.make_async_copy(src, dst, s_load.at[n])
        for n, (src, dst) in enumerate(
            [(right_hbm, right_ref), (core_hbm, core_ref), (gauss_hbm, gauss_ref), (left_hbm, left_ref)]
        )
    ]
    for load in loads:
        load.start()

    def meet():
        tops = ((group < final) & owner).astype(jnp.int32)

        @pl.when(group == 0)
        def _():
            pl.semaphore_wait(barrier, size)

        @pl.when(group == 1)
        def _():
            pl.semaphore_wait(barrier, size + size * tops)

        @pl.when(group > 1)
        def _():
            pl.semaphore_wait(barrier, size - 1 + owners + size * tops)

    def remote(src, dst, send, recv, peer, to_group):
        return pltpu.make_async_remote_copy(
            src_ref=src,
            dst_ref=dst,
            send_sem=send,
            recv_sem=recv,
            device_id={"mode": peer, "cores": to_group},
            device_id_type=MESH,
        )

    def await_piece(dst_ref, recv):
        remote(dst_ref, dst_ref, recv, recv, partner(me, 1, size), group).wait_recv()

    def scatter(out_ref, in_ref, sends, recvs, to_group):
        return [
            remote(
                out_ref.at[pl.ds(c * LANES, extents[c])],
                in_ref.at[me, pl.ds(0, extents[c])],
                sends.at[c],
                recvs.at[me],
                first + c,
                to_group,
            )
            for c in range(owners)
        ]

    def each(order, home, act):
        for c in order:
            if home:
                act(c)
            else:
                pl.when(me != first + c)(lambda c=c: act(c))

    def scatter_start(copies, home):
        start = lambda c: copies[c].start()
        pl.when(me < size // 2)(lambda: each(range(owners - 1, -1, -1), home, start))
        pl.when(me >= size // 2)(lambda: each(range(owners), home, start))

    def scatter_sent(copies, home):
        each(range(owners), home, lambda c: copies[c].wait_send())

    def gathered(in_ref, recvs, extent, own=None):
        if own is None:
            value = None
        else:
            value = own[pl.ds(pl.multiple_of(mine * LANES, LANES), extent)].astype(F32)
        for d in everyone[0 if own is None else 1 :]:
            peer = partner(me, d, size)
            landing = in_ref.at[peer, pl.ds(0, extent)]
            await_piece(landing, recvs.at[peer])
            term = landing[...].astype(F32)
            value = term if value is None else value + term
        return value

    def spread(src_ref, dst_ref, sends, recvs, to_group, home):
        return [
            remote(src_ref, dst_ref, sends.at[d], recvs.at[mine], partner(me, d, size), to_group)
            for d in owner_first(size) + ([0] if home else [])
        ]

    def block(ref, extent):
        return ref.at[pl.ds(pl.multiple_of(mine * LANES, LANES), extent)]

    def owned(run):
        if extents[-1] == LANES:
            pl.when(owner)(lambda: run(LANES))
        else:
            pl.when(owner & (me < last))(lambda: run(LANES))
            pl.when(me == last)(lambda: run(extents[-1]))

    def relay(in_ref, recvs, piece_ref, buf_ref, sends, lands, own=None):
        def finish(extent):
            piece = piece_ref.at[pl.ds(0, extent)]
            copies = spread(piece, block(buf_ref, extent), sends, lands, group, False)
            with scope("part_gather"):
                piece[...] = gathered(in_ref, recvs, extent, own).astype(BF16)
            for copy in copies:
                copy.start()
            block(buf_ref, extent)[...] = piece[...]

        owned(finish)
        for c in range(owners):

            @pl.when(me != first + c)
            def _(c=c):
                await_piece(buf_ref.at[pl.ds(c * LANES, extents[c])], lands.at[c])

    def relayed(piece_ref, buf_ref, sends, lands):
        def finish(extent):
            piece = piece_ref.at[pl.ds(0, extent)]
            for copy in spread(piece, block(buf_ref, extent), sends, lands, group, False):
                copy.wait_send()

        owned(finish)

    def split():
        with scope("split"):
            for i in range(modes):
                slices[i] = core_ref[:, i, :]

    def contract(held):
        rows_buf[...] = dot(core_ref[...].reshape(rank * modes, rank), held, 1, 0)
        return [rows_buf[pl.ds(i, rank, stride=modes), :].astype(BF16) for i in range(modes)]

    def fold(partials):
        total = None
        for i in range(modes):
            term = dot(partials[i][:, :sketch], gauss[i], 1, 1)
            total = term if total is None else total + term
        part_out[pl.ds(0, rank), pl.ds(0, sketch)] = total.astype(part_out.dtype)

    def factor(total):
        row_id = lax.broadcasted_iota(jnp.int32, (wide, wide), 0)
        lane_id = lax.broadcasted_iota(jnp.int32, (wide, wide), 1)
        total = jnp.where((row_id == lane_id) & (row_id >= sketch), 1.0, total)
        with scope("chol"):
            return lower_inverse(total, sketch, 8)

    def emit_frames(image, inverse):
        orth = dot(image, inverse, 1, 1, EXACT) * scale
        for i in range(modes):
            rows_buf[pl.ds(i, tall, stride=modes), :] = orth[i * tall : (i + 1) * tall]
        frames = rows_buf[pl.ds(0, sketch * modes), :].astype(BF16)
        frames_ref[...] = frames[:, :sketch].reshape(sketch, modes, sketch)

    def emit_faces():
        faces = jnp.concatenate([carry_own[c] for c in range(owners)], axis=1)
        faces_ref[...] = faces[:sketch, :rank].astype(F32).reshape(sketch, 1, rank)

    blocks = [(r, c) for r in range(owners) for c in range(r + 1)]
    tops, place = [], 0
    for r, c in blocks:
        tops.append(place)
        place += extents[r]

    @pl.when(group == 0)
    def _():
        loads[1].wait()
        loads[3].wait()
        carry = left_ref[...].T.astype(BF16)
        carry = jnp.concatenate([carry, jnp.zeros((tall - sketch, rank), BF16)], axis=0)
        with scope("build0"):
            built = [dot(carry, core_ref[:, i, :], 1, 0).astype(BF16) for i in range(modes)]
            for i in range(modes):
                slices[i, pl.ds(0, tall)] = built[i]
            stack = jnp.concatenate(built, axis=0)
            square = dot(stack, stack, 0, 0)
            pad = owners * LANES - rank
            square = jnp.concatenate([square, jnp.zeros((rank, pad), F32)], axis=1)
            square = jnp.concatenate([square, jnp.zeros((pad, rank + pad), F32)], axis=0)
            for (r, c), top in zip(blocks, tops):
                wide_out[pl.ds(top, extents[r]), :] = square[
                    r * LANES : r * LANES + extents[r], c * LANES : (c + 1) * LANES
                ]
            if wide_out.shape[0] > place:
                wide_out[pl.ds(place, wide_out.shape[0] - place), :] = jnp.zeros(
                    (wide_out.shape[0] - place, LANES), F32
                )
        loads[0].wait()
        loads[2].wait()
        meet()
        copies = []
        for d in far_first(size) + [0]:
            peer = partner(me, d, size)
            copies.append(
                remote(
                    wide_out.at[pl.ds(pl.multiple_of(peer * share, 8), share)],
                    wide_in.at[me],
                    s_wide.at[d],
                    r_wide.at[me],
                    peer,
                    upward,
                )
            )
        for copy in copies:
            copy.start()
        with scope("twin0"):
            await_piece(head_buf, r_twin.at[0])
        held = head_buf[pl.ds(0, rank), :]
        image = jnp.concatenate(
            [dot(slices[i, pl.ds(0, tall)], held, 1, 0) for i in range(modes)], axis=0
        )
        await_piece(inv_in, r_twin.at[1])
        emit_frames(image, inv_in[...])
        with scope("twin2"):
            await_piece(carry_own, r_twin.at[2])
        emit_faces()
        for copy in copies:
            copy.wait_send()

    @pl.when(group > 0)
    def _():
        part_out[...] = jnp.zeros(part_out.shape, part_out.dtype)
        if proj_out.shape[0] > rank:
            proj_out[pl.ds(rank, proj_out.shape[0] - rank), :] = jnp.zeros(
                (proj_out.shape[0] - rank, wide), F32
            )
        loads[2].wait()
        for i in range(modes):
            gauss[i] = gauss_ref[:, i, :]
        loads[0].wait()
        loads[1].wait()
        loads[3].wait()

        @pl.when(group == final)
        def _():
            sketch_buf[...] = jnp.zeros(sketch_buf.shape, BF16)
            sketch_buf[pl.ds(0, rank), pl.ds(0, sketch)] = right_ref[...]

        @pl.when(group < final)
        def _():
            split()
            with scope("meet"):
                meet()

        all_copies = [
            remote(
                wide_piece,
                wide_all.at[pl.ds(pl.multiple_of(me * share, 8), share)],
                s_all.at[d],
                r_all.at[me],
                partner(me, d, size),
                group,
            )
            for d in far_first(size)
        ]

        @pl.when(group == 1)
        def _():
            value = None
            for d in everyone:
                peer = partner(me, d, size)
                with scope("wide_wait"):
                    await_piece(wide_in.at[peer], r_wide.at[peer])
                term = wide_in[peer]
                value = term if value is None else value + term
            wide_piece[...] = value
            for copy in all_copies:
                copy.start()
            wide_all[pl.ds(pl.multiple_of(me * share, 8), share)] = value

        @pl.when(group < final)
        def _():
            with scope("relay_sk"):
                relay(part_in, r_part, piece_sk, sketch_buf, s_sk, r_sk)

        with scope("mark"):
            held = sketch_buf[pl.ds(0, rank), :]
        partials = contract(held)
        fold(partials)

        @pl.when(group == final)
        def _():
            with scope("meet3"):
                meet()

        @pl.when(group > 1)
        def _():
            part_copies = scatter(part_out, part_in, s_part, r_part, down)
            scatter_start(part_copies, True)
            pl.when(group == final)(split)
            pl.when(group < final)(lambda: relayed(piece_sk, sketch_buf, s_sk, r_sk))
            scatter_sent(part_copies, True)
            with scope("wait_carry"):
                for c in range(owners):
                    await_piece(carry_buf.at[c], r_next.at[c])

        @pl.when(group == 1)
        def _():
            part_copies = scatter(part_out, head_in, s_part, r_head, group)
            scatter_start(part_copies, False)
            with scope("all_wait"):
                for d in everyone[1:]:
                    peer = partner(me, d, size)
                    await_piece(
                        wide_all.at[pl.ds(pl.multiple_of(peer * share, 8), share)], r_all.at[peer]
                    )
            with scope("unpack"):
                tile = {}
                for (r, c), top in zip(blocks, tops):
                    value = wide_all[pl.ds(top, extents[r]), :]
                    if extents[r] < LANES:
                        value = jnp.concatenate(
                            [value, jnp.zeros((LANES - extents[r], LANES), F32)], axis=0
                        )
                    tile[r, c] = value
                    if r > c:
                        tile[c, r] = value.T
                for r in range(owners):
                    row = jnp.concatenate([tile[r, c] for c in range(owners)], axis=1)
                    high = row.astype(BF16)
                    full_hi[pl.ds(r * LANES, LANES)] = high
                    full_lo[pl.ds(r * LANES, LANES)] = (row - high.astype(F32)).astype(BF16)
            with scope("relay_hd"):
                relay(head_in, r_head, piece_hd, head_buf, s_hd, r_hd, part_out)
            twins = [
                remote(src, dst, s_twin.at[n], r_twin.at[n], me, down)
                for n, (src, dst) in enumerate(
                    [(head_buf, head_buf), (inv_buf, inv_in), (carry_buf, carry_own)]
                )
            ]
            twins[0].start()
            with scope("image0"):
                held = head_buf[pl.ds(0, rank), :]
                spread_y = (
                    dot(full_hi[:, :rank], held, 1, 0) + dot(full_lo[:, :rank], held, 1, 0)
                )[:rank]
                high = spread_y.astype(BF16)
                low = (spread_y - high.astype(F32)).astype(BF16)
                terms = dot(held, jnp.concatenate([high, low], axis=1), 0, 0)
            inverse = factor(terms[:, :wide] + terms[:, wide:])
            inv_buf[...] = inverse
            twins[1].start()
            carry = dot(inverse, spread_y, 1, 1, EXACT)[:tall].astype(BF16)
            for c in range(owners):
                width = min(LANES, rank - c * LANES)
                if width < LANES:
                    carry_buf[c] = jnp.zeros((tall, LANES), BF16)
                carry_buf[c, :, pl.ds(0, width)] = carry[:, c * LANES : c * LANES + width]
            twins[2].start()
            relayed(piece_sk, sketch_buf, s_sk, r_sk)
            relayed(piece_hd, head_buf, s_hd, r_hd)
            scatter_sent(part_copies, False)
            for copy in all_copies:
                copy.wait_send()
            for twin in twins:
                twin.wait_send()

        carry = jnp.concatenate([carry_buf[c] for c in range(owners)], axis=1)[:, :rank]
        partials = [rows_buf[pl.ds(i, rank, stride=modes), :].astype(BF16) for i in range(modes)]
        gram_copies = [
            remote(
                gram_out, gram_in.at[me], s_gram.at[d], r_gram.at[me], partner(me, d, size), group
            )
            for d in far_first(size)
        ]
        proj_copies = scatter(proj_out, proj_in, s_proj, r_proj, group)
        images = [dot(carry, partials[i], 1, 0) for i in range(modes)]
        image = jnp.concatenate(images, axis=0)
        high = image.astype(BF16)
        low = (image - high.astype(F32)).astype(BF16)
        pair = jnp.concatenate([high, low], axis=1)
        terms = dot(high, pair, 0, 0)
        cross = terms[:, wide:]
        gram = terms[:, :wide] + cross + cross.T
        half, quarter = wide // 2, wide // 4
        lower_rows = gram_out.shape[0] - quarter
        gram_out[pl.ds(0, lower_rows), :] = gram[half : half + lower_rows]
        gram_out[pl.ds(lower_rows, quarter), :] = jnp.concatenate(
            [gram[:quarter, :half], gram[quarter:half, :half]], axis=1
        )
        with scope("gram_send"):
            for copy in gram_copies:
                copy.start()
        built = jnp.concatenate(
            [dot(carry, slices[i], 1, 0).astype(BF16) for i in range(modes)], axis=0
        )
        proj = dot(built, pair, 0, 0)
        proj_out[pl.ds(0, rank), :] = proj[:, :wide] + proj[:, wide:]
        scatter_start(proj_copies, False)
        gram_in[me] = gram_out[...]
        with scope("gram_wait"):
            for d in everyone[1:]:
                peer = partner(me, d, size)
                await_piece(gram_in.at[peer], r_gram.at[peer])
        total = None
        for source in range(size):
            term = gram_in[source]
            total = term if total is None else total + term
        lower = total[:lower_rows]
        if lower_rows < half:
            lower = jnp.concatenate([lower, jnp.zeros((half - lower_rows, wide), F32)], axis=0)
        corner = total[lower_rows:]
        corner = jnp.concatenate([corner[:, :half], corner[:, half:]], axis=0)
        upper = jnp.concatenate([corner, lower.T[:half]], axis=1)
        inverse = factor(jnp.concatenate([upper, lower], axis=0))

        next_copies = spread(piece_ca, carry_buf.at[mine], s_next, r_next, upward, True)
        own_copies = spread(piece_ca, carry_own.at[mine], s_own, r_own, group, False)

        def project(extent):
            with scope("proj_gather"):
                value = gathered(proj_in, r_proj, extent, proj_out)
            if extent < LANES:
                value = jnp.concatenate([value, jnp.zeros((LANES - extent, wide), F32)], axis=0)
            piece_ca[...] = dot(inverse, value, 1, 1, EXACT)[:tall].astype(BF16)

            @pl.when(group < final)
            def _():
                for copy in next_copies:
                    copy.start()

            for copy in own_copies:
                copy.start()
            carry_own[mine] = piece_ca[...]

        owned(project)
        emit_frames(image, inverse)
        scatter_sent(proj_copies, False)
        for copy in gram_copies:
            copy.wait_send()
        with scope("wait_own"):
            for c in range(owners):

                @pl.when(me != first + c)
                def _(c=c):
                    await_piece(carry_own.at[c], r_own.at[c])

        emit_faces()

        def drain():
            for copy in own_copies:
                copy.wait_send()

            @pl.when(group < final)
            def _():
                for copy in next_copies:
                    copy.wait_send()

        pl.when(owner)(drain)


def body(train_cores, sketch_cores, left_interface, right_sketch):
    size = lax.axis_size("mode")
    group_count = lax.axis_size("cores")
    _, rank, modes, _ = train_cores.shape
    sketch = sketch_cores.shape[1]
    wide, tall = up(sketch, LANES), up(sketch, 8)
    owners = -(-rank // LANES)
    deep = owners * LANES
    scale = math.sqrt(sketch * modes * size)
    dims = (size, group_count, rank, sketch, modes, owners, scale)
    gram_rows = up(max(sketch - wide // 2, 8), 8) + wide // 4
    packed = LANES * owners * (owners - 1) // 2 + owners * up(rank - LANES * (owners - 1), 16)
    share = up(-(-packed // size), 8)
    anywhere = pl.BlockSpec(memory_space=pl.ANY)
    vmem = pl.BlockSpec(memory_space=pltpu.VMEM)
    dma = pltpu.SemaphoreType.DMA((size,))
    frames, faces = pl.pallas_call(
        functools.partial(kernel, dims),
        out_shape=(
            jax.ShapeDtypeStruct((sketch, modes, sketch), BF16),
            jax.ShapeDtypeStruct((sketch, 1, rank), F32),
        ),
        in_specs=[anywhere] * 4,
        out_specs=(vmem, vmem),
        scratch_shapes=[
            pltpu.VMEM((rank, modes, rank), BF16),
            pltpu.VMEM((sketch, modes, sketch), BF16),
            pltpu.VMEM((rank, sketch), F32),
            pltpu.VMEM((rank, sketch), BF16),
            pltpu.VMEM((modes, rank, rank), BF16),
            pltpu.VMEM((modes, sketch, sketch), BF16),
            pltpu.VMEM((rank * modes, wide), F32),
            pltpu.VMEM((deep, wide), BF16),
            pltpu.VMEM((deep, wide), BF16),
            pltpu.VMEM((deep, wide), BF16),
            pltpu.VMEM((size, LANES, wide), BF16),
            pltpu.VMEM((size, LANES, wide), BF16),
            pltpu.VMEM((owners, tall, LANES), BF16),
            pltpu.VMEM((owners, tall, LANES), BF16),
            pltpu.VMEM((deep, wide), F32),
            pltpu.VMEM((size, LANES, wide), F32),
            pltpu.VMEM((gram_rows, wide), F32),
            pltpu.VMEM((size, gram_rows, wide), F32),
            pltpu.VMEM((LANES, wide), BF16),
            pltpu.VMEM((tall, LANES), BF16),
            pltpu.VMEM((LANES, wide), BF16),
            pltpu.VMEM((wide, wide), F32),
            pltpu.VMEM((wide, wide), F32),
            pltpu.VMEM((size * share, LANES), F32),
            pltpu.VMEM((size, share, LANES), F32),
            pltpu.VMEM((share, LANES), F32),
            pltpu.VMEM((size * share, LANES), F32),
            pltpu.VMEM((deep, deep), BF16),
            pltpu.VMEM((deep, deep), BF16),
        ]
        + [dma] * 22,
        compiler_params=pltpu.CompilerParams(collective_id=0, has_side_effects=True),
    )(train_cores[0], sketch_cores[0], left_interface.T, right_sketch)
    return frames[None], faces[:, 0][None]


def solution(mesh):
    in_specs = (P("cores", None, "mode", None), P("cores", None, "mode", None), P(), P())
    out_specs = (P("cores", None, "mode", None), P("cores", None, None))
    return jax.shard_map(body, mesh=mesh, in_specs=in_specs, out_specs=out_specs, check_vma=False)
```
